32 devices in a mesh: dp: 1 (over z), tp: 4 (over y), ep: 8 (over x, core).
Axes of the slice: x: 4, y: 4, z: 1, core: 2. Of those that a mesh axis runs over, the one named last changes fastest.
The devices are a block of a 4x4x8 slice.
Arguments:
- x: bfloat16 [4096, 2048], P(('dp', 'ep', 'tp'))
- idx: int32 [4096, 8], P(('dp', 'ep', 'tp'))
- gate: float32 [4096, 8], P(('dp', 'ep', 'tp'))
- w1: bfloat16 [128, 2048, 768], P('ep', None, 'tp')
- w3: bfloat16 [128, 2048, 768], P('ep', None, 'tp')
- w2: bfloat16 [128, 768, 2048], P('ep', 'tp')
Outputs:
- output: bfloat16 [4096, 2048], P(('dp', 'ep', 'tp'))
All inputs are finite; a program needn't handle non-finite values.
Results may differ from the reference program's by a relative error of at most 0.001.
Values are sent between devices in bfloat16 or wider.
A program may use at most 768 MiB of HBM per device.

```python
import jax
import jax.numpy as jnp
from jax import lax

D = 2048
FF = 768
EXPERTS = 128
TOP = 8
TOKENS_DEV = 128
EP = 8
TP = 4

ROWS = TOKENS_DEV * EP * TP
CAP = 8 * ((TOP * ROWS // EXPERTS + 9) // 8)


def _route(key):
    ndev = EP * TP
    nb = TOKENS_DEV // EP
    m = EXPERTS // EP
    k1 = (TOP + 1) // 2
    k2 = TOP - k1
    ka, kd, kt1, kt2, ks = jax.random.split(key, 5)
    a = jnp.argsort(jax.random.uniform(ka, (ndev, nb, EP)), axis=-1).astype(jnp.int32)
    shift = jax.random.randint(kd, (ndev, nb, 1), 1, EP)
    b = (a + shift) % EP
    r = (jnp.arange(ndev)[:, None] * nb + jnp.arange(nb)[None, :])[:, :, None]
    tau1 = jax.random.randint(kt1, (EP,), 0, m)
    tau2 = jax.random.randint(kt2, (EP,), 0, m)
    c1 = (r * k1 + tau1[a]) % m
    c2 = (r * k2 + tau2[b]) % m
    e1 = a[..., None] * m + (c1[..., None] + jnp.arange(k1)) % m
    e2 = b[..., None] * m + (c2[..., None] + jnp.arange(k2)) % m
    idx = jnp.concatenate([e1, e2], axis=-1).reshape(ROWS, TOP)
    perm = jnp.argsort(jax.random.uniform(ks, (ROWS, TOP)), axis=-1)
    return jnp.take_along_axis(idx, perm, axis=1).astype(jnp.int32)


def _weights(key, shape, fan_in):
    keys = jax.random.split(key, EXPERTS)
    return lax.map(lambda k: (jax.random.normal(k, shape, jnp.float32) * fan_in ** -0.5).astype(jnp.bfloat16), keys)


def setup_inputs(seed: int = 0, part: int = 0) -> dict:
    key = jax.random.PRNGKey(seed)
    k_shared, k_part = jax.random.split(key)
    kx, kr, kg = jax.random.split(jax.random.fold_in(k_part, part), 3)
    k1, k3, k2 = jax.random.split(k_shared, 3)
    x = jax.random.normal(kx, (ROWS, D), jnp.float32).astype(jnp.bfloat16)
    idx = _route(kr)
    gate = jax.nn.softmax(0.5 * jax.random.normal(kg, (ROWS, TOP), jnp.float32), axis=-1)
    return {'x': x, 'idx': idx, 'gate': gate,
            'w1': _weights(k1, (D, FF), D), 'w3': _weights(k3, (D, FF), D), 'w2': _weights(k2, (FF, D), FF)}


def reference(x, idx, gate, w1, w3, w2):
    flat = idx.reshape(-1)
    gflat = gate.reshape(-1)
    order = jnp.argsort(flat)
    counts = jnp.zeros((EXPERTS,), jnp.int32).at[flat].add(1)
    starts = jnp.cumsum(counts) - counts
    slot = jnp.arange(CAP)

    def body(acc, e_in):
        w1e, w3e, w2e, start, count = e_in
        pid = order[jnp.clip(start + slot, 0, flat.shape[0] - 1)]
        tok = pid // TOP
        g = jnp.where(slot < count, gflat[pid], 0.0)
        xe = x[tok]
        a = jnp.dot(xe, w1e, preferred_element_type=jnp.float32)
        b = jnp.dot(xe, w3e, preferred_element_type=jnp.float32)
        h = (jax.nn.silu(a) * b).astype(jnp.bfloat16)
        o = jnp.dot(h, w2e, preferred_element_type=jnp.float32)
        return acc.at[tok].add(o * g[:, None]), None

    acc, _ = lax.scan(body, jnp.zeros((ROWS, D), jnp.float32), (w1, w3, w2, starts, counts))
    return acc.astype(jnp.bfloat16)
```

```python
import functools

import jax
import jax.numpy as jnp
from jax import lax
from jax.experimental import pallas as pl
from jax.experimental.pallas import tpu as pltpu
from jax.sharding import PartitionSpec as P

MESH = pl.DeviceIdType.MESH
GATE_LANES = 128
SLOTS = 3


def _route(x, idx, gate, n_pos, n_exp, cap):
    rows = x.shape[0]
    pos = idx // n_exp
    hit = jnp.any(pos[:, None, :] == jnp.arange(n_pos)[None, :, None], axis=-1)
    r = jnp.arange(rows)
    before = (r[None, :] < r[:, None]).astype(jnp.bfloat16)
    rank = jnp.dot(before, hit.astype(jnp.bfloat16), preferred_element_type=jnp.float32).astype(jnp.int32)
    slot = jnp.where(hit, rank, cap)
    sel = slot.T[:, None, :] == jnp.arange(cap)[None, :, None]
    pick = sel.astype(jnp.bfloat16)
    xs = jnp.einsum('qsr,rd->qsd', pick, x, preferred_element_type=jnp.float32).astype(jnp.bfloat16)
    experts = jnp.arange(n_pos * n_exp)
    g = jnp.sum(jnp.where(idx[:, :, None] == experts[None, None, :], gate[:, :, None], 0.0), axis=1)
    hi = lax.reduce_precision(g, 8, 7)
    mid = lax.reduce_precision(g - hi, 8, 7)
    lo = g - hi - mid
    parts = jnp.stack([hi, mid, lo], axis=1).astype(jnp.bfloat16).reshape(rows, 3, n_pos, n_exp)
    gs = jnp.einsum('qsr,rpqe->qspe', pick, parts, preferred_element_type=jnp.float32)
    gs = gs.reshape(n_pos, cap, 3 * n_exp).astype(jnp.bfloat16)
    gs = jnp.pad(gs, ((0, 0), (0, 0), (0, GATE_LANES - 3 * n_exp)))
    return jnp.concatenate([xs, gs], axis=-1), sel


def _kernel(n_pos, n_tp, cap, xs, w1, w3, w2, out, xb, acc, rec, rel, b1, b3, b2,
            wsem, sx, rx, sy, ry, sr, rr, sc, rc, sf, rf):
    q = lax.axis_index('ep')
    y = lax.axis_index('tp')
    up = lax.rem(y + 1, n_tp)
    down = lax.rem(y + n_tp - 1, n_tp)
    n_exp, d, ff = w1.shape
    ch = n_pos * cap
    half = ch // 2
    steps = 4 * n_exp

    def weights(step):
        e, s = lax.rem(step, n_exp), lax.rem(step, SLOTS)
        return (pltpu.make_async_copy(w1.at[e], b1.at[s], wsem.at[s, 0]),
                pltpu.make_async_copy(w3.at[e], b3.at[s], wsem.at[s, 1]),
                pltpu.make_async_copy(w2.at[e], b2.at[s], wsem.at[s, 2]))

    def remote(src, dst, ssem, rsem, dev):
        return pltpu.make_async_remote_copy(src_ref=src, dst_ref=dst, send_sem=ssem, recv_sem=rsem,
                                            device_id=dev, device_id_type=MESH)

    for s in range(SLOTS - 1):
        for c in weights(s):
            c.start()

    barrier = pltpu.get_barrier_semaphore()
    for k in range(1, n_pos):
        pl.semaphore_signal(barrier, inc=1, device_id={'ep': lax.rem(q + k, n_pos)}, device_id_type=MESH)
    for t in (up, down):
        pl.semaphore_signal(barrier, inc=1, device_id={'tp': t}, device_id_type=MESH)
    pl.semaphore_wait(barrier, n_pos + 1)

    def blk(k):
        return pl.ds(k * cap, cap)

    def x_send(k):
        to = lax.rem(q + n_pos - k, n_pos)
        return remote(xs.at[to], xb.at[0, blk(k)], sx.at[k], rx.at[k], {'ep': to})

    def y_send(way, k):
        src = xs.at[q] if k == 0 else xb.at[0, blk(k)]
        if way == 0:
            return remote(src, xb.at[3, blk(k)], sy.at[0, k], ry.at[0, k], {'tp': up})
        return remote(src, xb.at[1, blk(k)], sy.at[1, k], ry.at[1, k], {'tp': down})

    def y_got(way, k):
        j = 3 if way == 0 else 1
        return remote(xb.at[j, blk(k)], xb.at[j, blk(k)], sy.at[way, k], ry.at[way, k], {'tp': up})

    def relay(way, i):
        if way == 1:
            b = blk(2 * i)
            return remote(xb.at[1, b], xb.at[2, b], sr.at[1, i], rr.at[1, i], {'tp': down})
        b = blk(2 * i + 1)
        return remote(xb.at[3, b], xb.at[2, b], sr.at[0, i], rr.at[0, i], {'tp': up})

    for k in range(1, n_pos):
        x_send(k).start()
    y_send(0, 0).start()
    y_send(1, 0).start()
    xb[0, blk(0)] = xs[q]
    for k in range(1, n_pos):
        x_send(k).wait_recv()
        y_send(0, k).start()
        y_send(1, k).start()

    lane = lax.broadcasted_iota(jnp.int32, (ch, GATE_LANES), 1)

    def chunk(j, order, hook=None):
        acc[j] = jnp.zeros((ch, d), jnp.float32)

        def expert(e, carry):
            step = order * n_exp + e
            s = lax.rem(step, SLOTS)

            @pl.when(step + SLOTS - 1 < steps)
            def _():
                for c in weights(step + SLOTS - 1):
                    c.start()
            for c in weights(step):
                c.wait()
            if hook is not None:
                hook(e)
            xv = xb[j, :, 0:d]
            a = jnp.dot(xv, b1[s], preferred_element_type=jnp.float32)
            b = jnp.dot(xv, b3[s], preferred_element_type=jnp.float32)
            h = (a * jax.nn.sigmoid(a) * b).astype(jnp.bfloat16)
            gv = xb[j, :, d:d + GATE_LANES].astype(jnp.float32)
            mine = (lane == e) | (lane == e + n_exp) | (lane == e + 2 * n_exp)
            g = jnp.sum(jnp.where(mine, gv, 0.0), axis=1, keepdims=True)
            wide = d // 4
            for n in range(4):
                cols = pl.ds(n * wide, wide)
                o = jnp.dot(h, b2[s, :, cols], preferred_element_type=jnp.float32)
                acc[j, :, cols] += g * o
            return carry

        lax.fori_loop(0, n_exp, expert, 0)

    quarter = n_exp // 4

    def relays(e):
        @pl.when(lax.rem(e, quarter) == quarter - 1)
        def _():
            i = e // quarter
            y_got(1, 2 * i).wait_recv()
            relay(1, i).start()
            y_got(0, 2 * i + 1).wait_recv()
            relay(0, i).start()

    lo, hi = pl.ds(0, half), pl.ds(half, half)

    c_up_hi = remote(acc.at[1, hi], rec.at[0, hi], sc.at[0], rc.at[0], {'tp': up})
    c_up_lo = remote(acc.at[1, lo], rec.at[0, lo], sc.at[1], rc.at[1], {'tp': up})
    c_dn_lo = remote(acc.at[3, lo], rec.at[1, lo], sc.at[2], rc.at[2], {'tp': down})
    c_dn_hi = remote(acc.at[3, hi], rec.at[1, hi], sc.at[3], rc.at[3], {'tp': down})
    c_far_lo = remote(acc.at[2, lo], rel.at[0], sc.at[4], rc.at[4], {'tp': up})
    c_far_hi = remote(acc.at[2, hi], rel.at[1], sc.at[5], rc.at[5], {'tp': down})

    chunk(0, 0, relays)
    for i in range(n_pos // 2):
        y_got(1, 2 * i + 1).wait_recv()
    chunk(1, 1)
    c_up_hi.start()
    for i in range(n_pos // 2):
        relay(0, i).wait_recv()
        relay(1, i).wait_recv()
    chunk(2, 2)
    c_far_lo.start()
    c_far_hi.start()
    for i in range(n_pos // 2):
        y_got(0, 2 * i).wait_recv()
    chunk(3, 3)
    c_dn_lo.start()
    c_far_lo.wait_recv()
    acc[1, lo] += rel[0]
    c_up_lo.start()
    c_far_hi.wait_recv()
    acc[3, hi] += rel[1]
    c_dn_hi.start()

    def f_send(k):
        to = lax.rem(q + k, n_pos)
        return remote(acc.at[0, blk(k)], out.at[q], sf.at[k], rf.at[k], {'ep': to})

    c_dn_lo.wait_recv()
    c_up_lo.wait_recv()
    acc[0, lo] += rec[0, lo] + rec[1, lo]
    for k in range(1, n_pos // 2):
        f_send(k).start()
    out[q] = acc[0, blk(0)]
    c_up_hi.wait_recv()
    c_dn_hi.wait_recv()
    acc[0, hi] += rec[0, hi] + rec[1, hi]
    for k in range(n_pos // 2, n_pos):
        f_send(k).start()

    for k in range(1, n_pos):
        x_send(k).wait_send()
    for k in range(n_pos):
        y_send(0, k).wait_send()
        y_send(1, k).wait_send()
    for i in range(n_pos // 2):
        relay(0, i).wait_send()
        relay(1, i).wait_send()
    for c in (c_up_hi, c_up_lo, c_dn_lo, c_dn_hi, c_far_lo, c_far_hi):
        c.wait_send()
    for k in range(1, n_pos):
        f_send(k).wait_send()
        f_send(k).wait_recv()


def _moe(xs, w1, w3, w2, n_pos, n_tp, cap):
    n_exp, d, ff = w1.shape
    ch = n_pos * cap
    wide = xs.shape[-1]
    dma = pltpu.SemaphoreType.DMA
    vmem = pl.BlockSpec(memory_space=pltpu.VMEM)
    hbm = pl.BlockSpec(memory_space=pl.ANY)
    return pl.pallas_call(
        functools.partial(_kernel, n_pos, n_tp, cap),
        out_shape=jax.ShapeDtypeStruct((n_pos, cap, d), jnp.float32),
        in_specs=[vmem, hbm, hbm, hbm],
        out_specs=vmem,
        scratch_shapes=[
            pltpu.VMEM((4, ch, wide), jnp.bfloat16),
            pltpu.VMEM((4, ch, d), jnp.float32),
            pltpu.VMEM((2, ch, d), jnp.float32),
            pltpu.VMEM((2, ch // 2, d), jnp.float32),
            pltpu.VMEM((SLOTS, d, ff), jnp.bfloat16),
            pltpu.VMEM((SLOTS, d, ff), jnp.bfloat16),
            pltpu.VMEM((SLOTS, ff, d), jnp.bfloat16),
            dma((SLOTS, 3)),
            dma((n_pos,)), dma((n_pos,)),
            dma((2, n_pos)), dma((2, n_pos)),
            dma((2, n_pos // 2)), dma((2, n_pos // 2)),
            dma((6,)), dma((6,)),
            dma((n_pos,)), dma((n_pos,)),
        ],
        compiler_params=pltpu.CompilerParams(
            collective_id=0, has_side_effects=True, vmem_limit_bytes=60 * 1024 * 1024),
    )(xs, w1, w3, w2)


def solution(mesh):
    n_pos, n_tp = mesh.shape['ep'], mesh.shape['tp']
    rows_spec = P(('dp', 'ep', 'tp'), None)

    def body(x, idx, gate, w1, w3, w2):
        rows, d = x.shape
        n_exp = w1.shape[0]
        cap = 2 * rows // n_pos
        xs, sel = _route(x, idx, gate, n_pos, n_exp, cap)
        back = _moe(xs, w1, w3, w2, n_pos, n_tp, cap)
        y = jnp.einsum('qsr,qsd->rd', sel.astype(jnp.float32), back,
                       precision=lax.Precision.HIGHEST, preferred_element_type=jnp.float32)
        return y.astype(jnp.bfloat16)

    return jax.shard_map(body, mesh=mesh,
                         in_specs=(rows_spec, rows_spec, rows_spec,
                                   P('ep', None, 'tp'), P('ep', None, 'tp'), P('ep', 'tp', None)),
                         out_specs=rows_spec, check_vma=False)
```

```python
import functools

import jax
import jax.numpy as jnp
from jax import lax
from jax.experimental import pallas as pl
from jax.experimental.pallas import tpu as pltpu
from jax.sharding import PartitionSpec as P

MESH = pl.DeviceIdType.MESH
GATE_LANES = 128


def _route(x, idx, gate, n_pos, n_exp, cap):
    rows = x.shape[0]
    pos = idx // n_exp
    hit = jnp.any(pos[:, None, :] == jnp.arange(n_pos)[None, :, None], axis=-1)
    r = jnp.arange(rows)
    before = (r[None, :] < r[:, None]).astype(jnp.bfloat16)
    rank = jnp.dot(before, hit.astype(jnp.bfloat16), preferred_element_type=jnp.float32).astype(jnp.int32)
    slot = jnp.where(hit, rank, cap)
    sel = slot.T[:, None, :] == jnp.arange(cap)[None, :, None]
    pick = sel.astype(jnp.bfloat16)
    xs = jnp.einsum('qsr,rd->qsd', pick, x, preferred_element_type=jnp.float32).astype(jnp.bfloat16)
    experts = jnp.arange(n_pos * n_exp)
    g = jnp.sum(jnp.where(idx[:, :, None] == experts[None, None, :], gate[:, :, None], 0.0), axis=1)
    hi = lax.reduce_precision(g, 8, 7)
    mid = lax.reduce_precision(g - hi, 8, 7)
    lo = g - hi - mid
    parts = jnp.stack([hi, mid, lo], axis=1).astype(jnp.bfloat16).reshape(rows, 3, n_pos, n_exp)
    gs = jnp.einsum('qsr,rpqe->qspe', pick, parts, preferred_element_type=jnp.float32)
    gs = gs.reshape(n_pos, cap, 3 * n_exp).astype(jnp.bfloat16)
    gs = jnp.pad(gs, ((0, 0), (0, 0), (0, GATE_LANES - 3 * n_exp)))
    return jnp.concatenate([xs, gs], axis=-1), sel


def _kernel(n_pos, n_tp, cap, xs, w1, w3, w2, out, xb, xt, acc, rec, rel, b13, b2,
            wsem, sx, rx, sn, rn, sl, rl, sr, rr, su, ru, sg, rg, sm, rm, sf, rf):
    q = lax.axis_index('ep')
    y = lax.axis_index('tp')
    up = lax.rem(y + 1, n_tp)
    down = lax.rem(y + n_tp - 1, n_tp)
    n_exp, ff, d = w1.shape
    ch = n_pos * cap
    half = ch // 2
    nh = n_pos // 2
    pairs = n_exp // 2

    def remote(src, dst, ssem, rsem, dev):
        return pltpu.make_async_remote_copy(src_ref=src, dst_ref=dst, send_sem=ssem, recv_sem=rsem,
                                            device_id=dev, device_id_type=MESH)

    def weights(e):
        i, r = e // 2, (e % 2) * 2 * ff
        return (pltpu.make_async_copy(w1.at[e], b13.at[i, pl.ds(r, ff)], wsem.at[e, 0]),
                pltpu.make_async_copy(w3.at[e], b13.at[i, pl.ds(r + ff, ff)], wsem.at[e, 1]),
                pltpu.make_async_copy(w2.at[e], b2.at[e], wsem.at[e, 2]))

    barrier = pltpu.get_barrier_semaphore()
    for k in range(1, n_pos):
        pl.semaphore_signal(barrier, inc=1, device_id={'ep': lax.rem(q + k, n_pos)}, device_id_type=MESH)
    for t in (up, down):
        pl.semaphore_signal(barrier, inc=1, device_id={'tp': t}, device_id_type=MESH)

    def load(e, carry):
        for c in weights(e):
            c.start()
        return carry

    lax.fori_loop(0, n_exp, load, 0)
    pl.semaphore_wait(barrier, n_pos + 1)

    def off(b):
        return b if b < nh else n_pos + nh - 1 - b

    def rows(n):
        return pl.ds(n * cap, cap)

    order = [b for r in range(nh) for b in (r, nh + r)]

    def x_send(b):
        to = lax.rem(q + n_pos - off(b), n_pos)
        return remote(xs.at[to], xb.at[0, rows(b)], sx.at[b], rx.at[b], {'ep': to})

    def near(b):
        src = xs.at[q] if b == 0 else xb.at[0, rows(b)]
        if b < nh:
            return remote(src, xb.at[1, rows(nh + b)], sn.at[b], rn.at[b], {'tp': up})
        return remote(src, xb.at[1, rows(b - nh)], sn.at[b], rn.at[b], {'tp': down})

    def late(r, way):
        if way == 0:
            return remote(xb.at[0, rows(r)], xb.at[3, rows(r)], sl.at[r], rl.at[r], {'tp': down})
        return remote(xb.at[0, rows(nh + r)], xb.at[3, rows(nh + r)], sl.at[nh + r], rl.at[nh + r], {'tp': up})

    def relay(r, way):
        if way == 0:
            return remote(xb.at[1, rows(nh + r)], xb.at[2, rows(r)], sr.at[r], rr.at[r], {'tp': up})
        return remote(xb.at[1, rows(r)], xb.at[2, rows(nh + r)], sr.at[nh + r], rr.at[nh + r], {'tp': down})

    def near_got(r, way):
        if way == 0:
            return remote(xb.at[1, rows(nh + r)], xb.at[1, rows(nh + r)], sn.at[r], rn.at[r], {'tp': up})
        return remote(xb.at[1, rows(r)], xb.at[1, rows(r)], sn.at[nh + r], rn.at[nh + r], {'tp': down})

    for b in order[1:]:
        x_send(b).start()
    near(0).start()
    xb[0, rows(0)] = xs[q]
    for b in order[1:]:
        x_send(b).wait_recv()
        near(b).start()

    lane = lax.broadcasted_iota(jnp.int32, (ch, GATE_LANES), 1)

    def unit(u, hook=None):
        acc[u] = jnp.zeros((ch, d), jnp.float32)
        wide = d // 4
        for n in range(4):
            cols = pl.ds(n * wide, wide)
            xt[cols, :] = xb[u, :, cols].T

        def gate(gv, e):
            mine = (lane == e) | (lane == e + n_exp) | (lane == e + 2 * n_exp)
            return jnp.sum(jnp.where(mine, gv, 0.0), axis=1, keepdims=True)

        def pair(i, carry):
            if hook is not None:
                hook(i)
            ab = jnp.dot(b13[i], xt[...], preferred_element_type=jnp.float32)
            gv = xb[u, :, d:d + GATE_LANES].astype(jnp.float32)
            h, g = [], []
            for t in range(2):
                a, b = ab[2 * t * ff:(2 * t + 1) * ff], ab[(2 * t + 1) * ff:(2 * t + 2) * ff]
                h.append((a * jax.nn.sigmoid(a) * b).astype(jnp.bfloat16).T)
                g.append(gate(gv, 2 * i + t))
            for n in range(4):
                cols = pl.ds(n * wide, wide)
                o0 = jnp.dot(h[0], b2[2 * i, :, cols], preferred_element_type=jnp.float32)
                o1 = jnp.dot(h[1], b2[2 * i + 1, :, cols], preferred_element_type=jnp.float32)
                acc[u, :, cols] += g[0] * o0 + g[1] * o1
            return carry

        lax.fori_loop(0, pairs, pair, 0)

    def first(i):
        for t in range(2):
            for c in weights(2 * i + t):
                c.wait()

        @pl.when(i < n_pos)
        def _():
            r = i // 2

            @pl.when(lax.rem(i, 2) == 0)
            def _():
                near_got(r, 0).wait_recv()
                relay(r, 0).start()
                late(r, 0).start()

            @pl.when(lax.rem(i, 2) == 1)
            def _():
                near_got(r, 1).wait_recv()
                relay(r, 1).start()
                late(r, 1).start()

    unit(0, first)
    unit(1)

    def plain(b):
        if b < nh:
            return remote(acc.at[1, rows(nh + b)], rec.at[1, rows(b)], su.at[b], ru.at[b], {'tp': down})
        return remote(acc.at[1, rows(b - nh)], rec.at[0, rows(b)], su.at[b], ru.at[b], {'tp': up})

    def far(b):
        return remote(acc.at[2, rows(b)], rel.at[rows(b)], sg.at[b], rg.at[b], {'tp': up if b < nh else down})

    def merged(b):
        w = 0 if b < nh else 1
        return remote(acc.at[3, rows(b)], rec.at[w, rows(b)], sm.at[b], rm.at[b], {'tp': down if w else up})

    def final(b):
        to = lax.rem(q + off(b), n_pos)
        return remote(acc.at[0, rows(b)], out.at[q], sf.at[b], rf.at[b], {'ep': to})

    back = [b for r in range(nh - 1, -1, -1) for b in (r, nh + r)]
    for b in back:
        plain(b).start()
    for r in range(nh):
        for w in range(2):
            relay(r, w).wait_recv()
    unit(2)
    for b in back:
        far(b).start()
    for r in range(nh):
        for w in range(2):
            late(r, w).wait_recv()
    unit(3)
    for b in back:
        far(b).wait_recv()
        acc[3, rows(b)] += rel[rows(b)]
        merged(b).start()
    for b in back:
        plain(b).wait_recv()
        merged(b).wait_recv()
        acc[0, rows(b)] += rec[0, rows(b)] + rec[1, rows(b)]
        if b:
            final(b).start()
        else:
            out[q] = acc[0, rows(b)]

    for b in range(n_pos):
        near(b).wait_send()
        plain(b).wait_send()
        far(b).wait_send()
        merged(b).wait_send()
        if b:
            x_send(b).wait_send()
            final(b).wait_send()
            final(b).wait_recv()
    for r in range(nh):
        for w in range(2):
            late(r, w).wait_send()
            relay(r, w).wait_send()


def _moe(xs, w1, w3, w2, n_pos, n_tp, cap):
    n_exp, ff, d = w1.shape
    ch = n_pos * cap
    wide = xs.shape[-1]
    dma = pltpu.SemaphoreType.DMA
    vmem = pl.BlockSpec(memory_space=pltpu.VMEM)
    hbm = pl.BlockSpec(memory_space=pl.ANY)
    return pl.pallas_call(
        functools.partial(_kernel, n_pos, n_tp, cap),
        out_shape=jax.ShapeDtypeStruct((n_pos, cap, d), jnp.float32),
        in_specs=[vmem, hbm, hbm, hbm],
        out_specs=vmem,
        scratch_shapes=[
            pltpu.VMEM((4, ch, wide), jnp.bfloat16),
            pltpu.VMEM((d, ch), jnp.bfloat16),
            pltpu.VMEM((4, ch, d), jnp.float32),
            pltpu.VMEM((2, ch, d), jnp.float32),
            pltpu.VMEM((ch, d), jnp.float32),
            pltpu.VMEM((n_exp // 2, 4 * ff, d), jnp.bfloat16),
            pltpu.VMEM((n_exp, ff, d), jnp.bfloat16),
            dma((n_exp, 3)),
        ] + [dma((n_pos,)) for _ in range(16)],
        compiler_params=pltpu.CompilerParams(
            collective_id=0, has_side_effects=True, vmem_limit_bytes=67043328),
    )(xs, w1, w3, w2)


def solution(mesh):
    n_pos, n_tp = mesh.shape['ep'], mesh.shape['tp']
    rows_spec = P(('dp', 'ep', 'tp'), None)

    def body(x, idx, gate, w1, w3, w2):
        rows, d = x.shape
        n_exp = w1.shape[0]
        cap = 2 * rows // n_pos
        xs, sel = _route(x, idx, gate, n_pos, n_exp, cap)
        back = _moe(xs, jnp.swapaxes(w1, 1, 2), jnp.swapaxes(w3, 1, 2), w2, n_pos, n_tp, cap)
        y = jnp.einsum('qsr,qsd->rd', sel.astype(jnp.float32), back,
                       precision=lax.Precision.HIGHEST, preferred_element_type=jnp.float32)
        return y.astype(jnp.bfloat16)

    return jax.shard_map(body, mesh=mesh,
                         in_specs=(rows_spec, rows_spec, rows_spec,
                                   P('ep', None, 'tp'), P('ep', None, 'tp'), P('ep', 'tp', None)),
                         out_specs=rows_spec, check_vma=False)
```

```python
import functools

import jax
import jax.numpy as jnp
from jax import lax
from jax.experimental import pallas as pl
from jax.experimental.pallas import tpu as pltpu
from jax.sharding import PartitionSpec as P

MESH = pl.DeviceIdType.MESH
GATE_LANES = 128


def _route(x, idx, gate, n_pos, n_exp, cap):
    rows = x.shape[0]
    pos = idx // n_exp
    hit = jnp.any(pos[:, None, :] == jnp.arange(n_pos)[None, :, None], axis=-1)
    r = jnp.arange(rows)
    before = (r[None, :] < r[:, None]).astype(jnp.bfloat16)
    rank = jnp.dot(before, hit.astype(jnp.bfloat16), preferred_element_type=jnp.float32).astype(jnp.int32)
    slot = jnp.where(hit, rank, cap)
    sel = slot.T[:, None, :] == jnp.arange(cap)[None, :, None]
    pick = sel.astype(jnp.bfloat16)
    xs = jnp.einsum('qsr,rd->qsd', pick, x, preferred_element_type=jnp.float32).astype(jnp.bfloat16)
    experts = jnp.arange(n_pos * n_exp)[:, None]
    ids, gates = idx.T, gate.T
    g = sum(jnp.where(ids[k][None, :] == experts, gates[k][None, :], 0.0) for k in range(idx.shape[1]))
    hi = lax.reduce_precision(g, 8, 7)
    mid = lax.reduce_precision(g - hi, 8, 7)
    lo = g - hi - mid
    parts = jnp.stack([hi, mid, lo]).astype(jnp.bfloat16).reshape(3, n_pos, n_exp, rows)
    gs = jnp.einsum('qsr,pqer->qspe', pick, parts, preferred_element_type=jnp.float32)
    gs = gs.reshape(n_pos, cap, 3 * n_exp).astype(jnp.bfloat16)
    gs = jnp.pad(gs, ((0, 0), (0, 0), (0, GATE_LANES - 3 * n_exp)))
    return jnp.concatenate([xs, gs], axis=-1), sel


def _kernel(n_pos, n_tp, cap, xs, w1, w3, w2, out, xb, xt, hs, acc, rec, rel, b13, b2,
            wsem, sx, rx, sn, rn, sl, rl, sr, rr, su, ru, sg, rg, sm, rm, sf, rf):
    q = lax.axis_index('ep')
    y = lax.axis_index('tp')
    up = lax.rem(y + 1, n_tp)
    down = lax.rem(y + n_tp - 1, n_tp)
    n_exp, ff, d = w1.shape
    ch = n_pos * cap
    half = ch // 2
    nh = n_pos // 2
    pairs = n_exp // 2

    def remote(src, dst, ssem, rsem, dev):
        return pltpu.make_async_remote_copy(src_ref=src, dst_ref=dst, send_sem=ssem, recv_sem=rsem,
                                            device_id=dev, device_id_type=MESH)

    def weights(e):
        i, r = e // 2, (e % 2) * 2 * ff
        return (pltpu.make_async_copy(w1.at[e], b13.at[i, pl.ds(r, ff)], wsem.at[e, 0]),
                pltpu.make_async_copy(w3.at[e], b13.at[i, pl.ds(r + ff, ff)], wsem.at[e, 1]),
                pltpu.make_async_copy(w2.at[e], b2.at[e], wsem.at[e, 2]))

    barrier = pltpu.get_barrier_semaphore()
    for k in range(1, n_pos):
        pl.semaphore_signal(barrier, inc=1, device_id={'ep': lax.rem(q + k, n_pos)}, device_id_type=MESH)
    for t in (up, down):
        pl.semaphore_signal(barrier, inc=1, device_id={'tp': t}, device_id_type=MESH)

    def load(e, carry):
        for c in weights(e):
            c.start()
        return carry

    lax.fori_loop(0, n_exp, load, 0)
    pl.semaphore_wait(barrier, n_pos + 1)

    def off(b):
        return b if b < nh else n_pos + nh - 1 - b

    def rows(n):
        return pl.ds(n * cap, cap)

    order = [b for r in range(nh) for b in (r, nh + r)]

    def x_send(b):
        to = lax.rem(q + n_pos - off(b), n_pos)
        return remote(xs.at[to], xb.at[0, rows(b)], sx.at[b], rx.at[b], {'ep': to})

    def near(b):
        src = xs.at[q] if b == 0 else xb.at[0, rows(b)]
        if b < nh:
            return remote(src, xb.at[1, rows(nh + b)], sn.at[b], rn.at[b], {'tp': up})
        return remote(src, xb.at[1, rows(b - nh)], sn.at[b], rn.at[b], {'tp': down})

    def late(r, way):
        if way == 0:
            return remote(xb.at[0, rows(r)], xb.at[3, rows(r)], sl.at[r], rl.at[r], {'tp': down})
        return remote(xb.at[0, rows(nh + r)], xb.at[3, rows(nh + r)], sl.at[nh + r], rl.at[nh + r], {'tp': up})

    def relay(r, way):
        if way == 0:
            return remote(xb.at[1, rows(nh + r)], xb.at[2, rows(r)], sr.at[r], rr.at[r], {'tp': up})
        return remote(xb.at[1, rows(r)], xb.at[2, rows(nh + r)], sr.at[nh + r], rr.at[nh + r], {'tp': down})

    def near_got(r, way):
        if way == 0:
            return remote(xb.at[1, rows(nh + r)], xb.at[1, rows(nh + r)], sn.at[r], rn.at[r], {'tp': up})
        return remote(xb.at[1, rows(r)], xb.at[1, rows(r)], sn.at[nh + r], rn.at[nh + r], {'tp': down})

    for b in order[1:]:
        x_send(b).start()
    near(0).start()
    xb[0, rows(0)] = xs[q]
    for b in order[1:]:
        x_send(b).wait_recv()
        near(b).start()

    lane = lax.broadcasted_iota(jnp.int32, (ch, GATE_LANES), 1)

    def unit(u, hook=None):
        acc[u] = jnp.zeros((ch, d), jnp.float32)
        wide = d // 4
        for n in range(4):
            cols = pl.ds(n * wide, wide)
            xt[cols, :] = xb[u, :, cols].T

        def gate(gv, e):
            mine = (lane == e) | (lane == e + n_exp) | (lane == e + 2 * n_exp)
            return jnp.sum(jnp.where(mine, gv, 0.0), axis=1, keepdims=True)

        def up_proj(i):
            if hook is not None:
                hook(i)
            return jnp.dot(b13[i], xt[...], preferred_element_type=jnp.float32)

        def hidden(i, ab):
            for t in range(2):
                a, b = ab[2 * t * ff:(2 * t + 1) * ff], ab[(2 * t + 1) * ff:(2 * t + 2) * ff]
                hs[lax.rem(i, 2), t] = (a * jax.nn.sigmoid(a) * b).astype(jnp.bfloat16).T

        def down_proj(i):
            gv = xb[u, :, d:d + GATE_LANES].astype(jnp.float32)
            g0, g1 = gate(gv, 2 * i), gate(gv, 2 * i + 1)
            p = lax.rem(i, 2)
            for n in range(4):
                cols = pl.ds(n * wide, wide)
                o0 = jnp.dot(hs[p, 0], b2[2 * i, :, cols], preferred_element_type=jnp.float32)
                o1 = jnp.dot(hs[p, 1], b2[2 * i + 1, :, cols], preferred_element_type=jnp.float32)
                acc[u, :, cols] += g0 * o0 + g1 * o1

        def pair(i, carry):
            ab = up_proj(i + 1)
            down_proj(i)
            hidden(i + 1, ab)
            return carry

        hidden(0, up_proj(0))
        lax.fori_loop(0, pairs - 1, pair, 0)
        down_proj(pairs - 1)

    def first(i):
        for t in range(2):
            for c in weights(2 * i + t):
                c.wait()

        @pl.when(i < n_pos)
        def _():
            r = i // 2

            @pl.when(lax.rem(i, 2) == 0)
            def _():
                near_got(r, 0).wait_recv()
                relay(r, 0).start()
                late(r, 0).start()

            @pl.when(lax.rem(i, 2) == 1)
            def _():
                near_got(r, 1).wait_recv()
                relay(r, 1).start()
                late(r, 1).start()

    unit(0, first)
    unit(1)

    def plain(b):
        if b < nh:
            return remote(acc.at[1, rows(nh + b)], rec.at[1, rows(b)], su.at[b], ru.at[b], {'tp': down})
        return remote(acc.at[1, rows(b - nh)], rec.at[0, rows(b)], su.at[b], ru.at[b], {'tp': up})

    def far(b):
        return remote(acc.at[2, rows(b)], rel.at[rows(b)], sg.at[b], rg.at[b], {'tp': up if b < nh else down})

    def merged(b):
        w = 0 if b < nh else 1
        return remote(acc.at[3, rows(b)], rec.at[w, rows(b)], sm.at[b], rm.at[b], {'tp': down if w else up})

    def final(b):
        to = lax.rem(q + off(b), n_pos)
        return remote(acc.at[0, rows(b)], out.at[q], sf.at[b], rf.at[b], {'ep': to})

    back = [b for r in range(nh - 1, -1, -1) for b in (r, nh + r)]
    for b in back:
        plain(b).start()
    for r in range(nh):
        for w in range(2):
            relay(r, w).wait_recv()
    unit(2)
    for b in back:
        far(b).start()
    for r in range(nh):
        for w in range(2):
            late(r, w).wait_recv()
    unit(3)
    for b in back:
        far(b).wait_recv()
        acc[3, rows(b)] += rel[rows(b)]
        merged(b).start()
    for b in back:
        plain(b).wait_recv()
        merged(b).wait_recv()
        acc[0, rows(b)] += rec[0, rows(b)] + rec[1, rows(b)]
        if b:
            final(b).start()
        else:
            out[q] = acc[0, rows(b)]

    for b in range(n_pos):
        near(b).wait_send()
        plain(b).wait_send()
        far(b).wait_send()
        merged(b).wait_send()
        if b:
            x_send(b).wait_send()
            final(b).wait_send()
            final(b).wait_recv()
    for r in range(nh):
        for w in range(2):
            late(r, w).wait_send()
            relay(r, w).wait_send()


def _moe(xs, w1, w3, w2, n_pos, n_tp, cap):
    n_exp, ff, d = w1.shape
    ch = n_pos * cap
    wide = xs.shape[-1]
    dma = pltpu.SemaphoreType.DMA
    vmem = pl.BlockSpec(memory_space=pltpu.VMEM)
    hbm = pl.BlockSpec(memory_space=pl.ANY)
    return pl.pallas_call(
        functools.partial(_kernel, n_pos, n_tp, cap),
        out_shape=jax.ShapeDtypeStruct((n_pos, cap, d), jnp.float32),
        in_specs=[vmem, hbm, hbm, hbm],
        out_specs=vmem,
        scratch_shapes=[
            pltpu.VMEM((4, ch, wide), jnp.bfloat16),
            pltpu.VMEM((d, ch), jnp.bfloat16),
            pltpu.VMEM((2, 2, ch, ff), jnp.bfloat16),
            pltpu.VMEM((4, ch, d), jnp.float32),
            pltpu.VMEM((2, ch, d), jnp.float32),
            pltpu.VMEM((ch, d), jnp.float32),
            pltpu.VMEM((n_exp // 2, 4 * ff, d), jnp.bfloat16),
            pltpu.VMEM((n_exp, ff, d), jnp.bfloat16),
            dma((n_exp, 3)),
        ] + [dma((n_pos,)) for _ in range(16)],
        compiler_params=pltpu.CompilerParams(
            collective_id=0, has_side_effects=True, vmem_limit_bytes=67043328),
    )(xs, w1, w3, w2)


def solution(mesh):
    n_pos, n_tp = mesh.shape['ep'], mesh.shape['tp']
    rows_spec = P(('dp', 'ep', 'tp'), None)

    def body(x, idx, gate, w1, w3, w2):
        rows, d = x.shape
        n_exp = w1.shape[0]
        cap = 2 * rows // n_pos
        xs, sel = _route(x, idx, gate, n_pos, n_exp, cap)
        back = _moe(xs, jnp.swapaxes(w1, 1, 2), jnp.swapaxes(w3, 1, 2), w2, n_pos, n_tp, cap)
        y = jnp.einsum('qsr,qsd->rd', sel.astype(jnp.float32), back,
                       precision=lax.Precision.HIGHEST, preferred_element_type=jnp.float32)
        return y.astype(jnp.bfloat16)

    return jax.shard_map(body, mesh=mesh,
                         in_specs=(rows_spec, rows_spec, rows_spec,
                                   P('ep', None, 'tp'), P('ep', None, 'tp'), P('ep', 'tp', None)),
                         out_specs=rows_spec, check_vma=False)
```

```python
import functools

import jax
import jax.numpy as jnp
from jax import lax
from jax.experimental import pallas as pl
from jax.experimental.pallas import tpu as pltpu
from jax.sharding import PartitionSpec as P

MESH = pl.DeviceIdType.MESH
GATE_LANES = 128
CODE_MAX = 32700.0
TINY = 1e-37


def _route(idx, gate, n_pos, n_exp, cap):
    rows = idx.shape[0]
    pos = idx // n_exp
    hit = jnp.any(pos[:, None, :] == jnp.arange(n_pos)[None, :, None], axis=-1)
    r = jnp.arange(rows)
    before = (r[None, :] < r[:, None]).astype(jnp.bfloat16)
    rank = jnp.dot(before, hit.astype(jnp.bfloat16), preferred_element_type=jnp.float32).astype(jnp.int32)
    slot = jnp.where(hit, rank, cap)
    sel = slot.T[:, None, :] == jnp.arange(cap)[None, :, None]
    pick = sel.astype(jnp.bfloat16)
    experts = jnp.arange(n_pos * n_exp)[:, None]
    ids, gates = idx.T, gate.T
    g = sum(jnp.where(ids[k][None, :] == experts, gates[k][None, :], 0.0) for k in range(idx.shape[1]))
    hi = lax.reduce_precision(g, 8, 7)
    mid = lax.reduce_precision(g - hi, 8, 7)
    lo = g - hi - mid
    parts = jnp.stack([hi, mid, lo]).astype(jnp.bfloat16).reshape(3, n_pos, n_exp, rows)
    gs = jnp.einsum('qsr,pqer->qspe', pick, parts, preferred_element_type=jnp.float32)
    gs = gs.reshape(n_pos, cap, 3 * n_exp).astype(jnp.bfloat16)
    gs = jnp.pad(gs, ((0, 0), (0, 0), (0, GATE_LANES - 3 * n_exp)))
    return pick.reshape(n_pos * cap, rows), gs.reshape(n_pos * cap, GATE_LANES)


def _encode(v):
    r, d = v.shape
    top = jnp.max(jnp.abs(v), axis=1, keepdims=True)
    e = jnp.ceil(jnp.log2(jnp.maximum(top, TINY)))
    root = v * lax.rsqrt(jnp.maximum(jnp.abs(v), TINY))
    code = jnp.round(root * (CODE_MAX * jnp.exp2(-0.5 * e))).astype(jnp.int32).astype(jnp.int16)
    return code, jnp.broadcast_to(e, (r, 128)).astype(jnp.int32).astype(jnp.int16)


def _decode(code, e):
    e = e.astype(jnp.int32).astype(jnp.float32)[:, 0:1]
    root = code.astype(jnp.int32).astype(jnp.float32) * (jnp.exp2(0.5 * e) * (1.0 / CODE_MAX))
    return root * jnp.abs(root)


def _kernel(n_pos, n_tp, cap, x, pick, gs, w1, w3, w2, out, xs, xb, xt, hs, acc, cd, rec, rel, fin, b13, b2,
            wsem, sx, rx, sn, rn, sl, rl, sr, rr, su, ru, sg, rg, sm, rm, sf, rf):
    q = lax.axis_index('ep')
    y = lax.axis_index('tp')
    up = lax.rem(y + 1, n_tp)
    down = lax.rem(y + n_tp - 1, n_tp)
    n_exp, ff, d = w1.shape
    ch = n_pos * cap
    half = ch // 2
    nh = n_pos // 2
    pairs = n_exp // 2

    def remote(src, dst, ssem, rsem, dev):
        return pltpu.make_async_remote_copy(src_ref=src, dst_ref=dst, send_sem=ssem, recv_sem=rsem,
                                            device_id=dev, device_id_type=MESH)

    def weights(e):
        i, r = e // 2, (e % 2) * 2 * ff
        return (pltpu.make_async_copy(w1.at[e], b13.at[i, pl.ds(r, ff)], wsem.at[e, 0]),
                pltpu.make_async_copy(w3.at[e], b13.at[i, pl.ds(r + ff, ff)], wsem.at[e, 1]),
                pltpu.make_async_copy(w2.at[e], b2.at[e], wsem.at[e, 2]))

    barrier = pltpu.get_barrier_semaphore()
    for k in range(1, n_pos):
        pl.semaphore_signal(barrier, inc=1, device_id={'ep': lax.rem(q + k, n_pos)}, device_id_type=MESH)
    for t in (up, down):
        pl.semaphore_signal(barrier, inc=1, device_id={'tp': t}, device_id_type=MESH)

    def load(e, carry):
        for c in weights(e):
            c.start()
        return carry

    lax.fori_loop(0, n_exp, load, 0)
    wide = d // 4
    for n in range(4):
        cols = pl.ds(n * wide, wide)
        picked = jnp.dot(pick[...], x[:, cols], preferred_element_type=jnp.float32)
        xs[:, :, cols] = picked.astype(jnp.bfloat16).reshape(n_pos, cap, wide)
    xs[:, :, d:d + GATE_LANES] = gs[...].reshape(n_pos, cap, GATE_LANES)
    pl.semaphore_wait(barrier, n_pos + 1)

    def off(b):
        return b if b < nh else n_pos + nh - 1 - b

    def rows(n):
        return pl.ds(n * cap, cap)

    order = [b for r in range(nh) for b in (r, nh + r)]

    def x_send(b):
        to = lax.rem(q + n_pos - off(b), n_pos)
        return remote(xs.at[to], xb.at[0, rows(b)], sx.at[b], rx.at[b], {'ep': to})

    def near(b):
        src = xs.at[q] if b == 0 else xb.at[0, rows(b)]
        if b < nh:
            return remote(src, xb.at[1, rows(nh + b)], sn.at[b], rn.at[b], {'tp': up})
        return remote(src, xb.at[1, rows(b - nh)], sn.at[b], rn.at[b], {'tp': down})

    def late(r, way):
        if way == 0:
            return remote(xb.at[0, rows(r)], xb.at[3, rows(r)], sl.at[r], rl.at[r], {'tp': down})
        return remote(xb.at[0, rows(nh + r)], xb.at[3, rows(nh + r)], sl.at[nh + r], rl.at[nh + r], {'tp': up})

    def relay(r, way):
        if way == 0:
            return remote(xb.at[1, rows(nh + r)], xb.at[2, rows(r)], sr.at[r], rr.at[r], {'tp': up})
        return remote(xb.at[1, rows(r)], xb.at[2, rows(nh + r)], sr.at[nh + r], rr.at[nh + r], {'tp': down})

    def near_got(r, way):
        if way == 0:
            return remote(xb.at[1, rows(nh + r)], xb.at[1, rows(nh + r)], sn.at[r], rn.at[r], {'tp': up})
        return remote(xb.at[1, rows(r)], xb.at[1, rows(r)], sn.at[nh + r], rn.at[nh + r], {'tp': down})

    for b in order[1:]:
        x_send(b).start()
    near(0).start()
    xb[0, rows(0)] = xs[q]
    for b in order[1:]:
        x_send(b).wait_recv()
        near(b).start()

    lane = lax.broadcasted_iota(jnp.int32, (ch, GATE_LANES), 1)

    def unit(u, hook=None):
        s = min(u, 1)
        acc[s] = jnp.zeros((ch, d), jnp.float32)
        for n in range(4):
            cols = pl.ds(n * wide, wide)
            xt[cols, :] = xb[u, :, cols].T

        def gate(gv, e):
            mine = (lane == e) | (lane == e + n_exp) | (lane == e + 2 * n_exp)
            return jnp.sum(jnp.where(mine, gv, 0.0), axis=1, keepdims=True)

        def up_proj(i):
            if hook is not None:
                hook(i)
            return jnp.dot(b13[i], xt[...], preferred_element_type=jnp.float32)

        def hidden(i, ab):
            for t in range(2):
                a, b = ab[2 * t * ff:(2 * t + 1) * ff], ab[(2 * t + 1) * ff:(2 * t + 2) * ff]
                hs[lax.rem(i, 2), t] = (a * jax.nn.sigmoid(a) * b).astype(jnp.bfloat16).T

        def down_proj(i):
            gv = xb[u, :, d:d + GATE_LANES].astype(jnp.float32)
            g0, g1 = gate(gv, 2 * i), gate(gv, 2 * i + 1)
            p = lax.rem(i, 2)
            for n in range(4):
                cols = pl.ds(n * wide, wide)
                o0 = jnp.dot(hs[p, 0], b2[2 * i, :, cols], preferred_element_type=jnp.float32)
                o1 = jnp.dot(hs[p, 1], b2[2 * i + 1, :, cols], preferred_element_type=jnp.float32)
                acc[s, :, cols] += g0 * o0 + g1 * o1

        def pair(i, carry):
            ab = up_proj(i + 1)
            down_proj(i)
            hidden(i + 1, ab)
            return carry

        hidden(0, up_proj(0))
        lax.fori_loop(0, pairs - 1, pair, 0)
        down_proj(pairs - 1)

    def first(i):
        for t in range(2):
            for c in weights(2 * i + t):
                c.wait()

        @pl.when(i < n_pos)
        def _():
            r = i // 2

            @pl.when(lax.rem(i, 2) == 0)
            def _():
                near_got(r, 0).wait_recv()
                relay(r, 0).start()
                late(r, 0).start()

            @pl.when(lax.rem(i, 2) == 1)
            def _():
                near_got(r, 1).wait_recv()
                relay(r, 1).start()
                late(r, 1).start()

    unit(0, first)
    unit(1)

    def encode(u, n, v):
        cd[u, rows(n), 0:d], cd[u, rows(n), d:d + 128] = _encode(v)

    def decode(ref):
        return _decode(ref[:, 0:d], ref[:, d:d + 128])

    def plain(b):
        if b < nh:
            return remote(cd.at[1, rows(nh + b)], rec.at[1, rows(b)], su.at[b], ru.at[b], {'tp': down})
        return remote(cd.at[1, rows(b - nh)], rec.at[0, rows(b)], su.at[b], ru.at[b], {'tp': up})

    def far(b):
        return remote(cd.at[2, rows(b)], rel.at[rows(b)], sg.at[b], rg.at[b], {'tp': up if b < nh else down})

    def merged(b):
        w = 0 if b < nh else 1
        return remote(cd.at[3, rows(b)], rec.at[w, rows(b)], sm.at[b], rm.at[b], {'tp': down if w else up})

    def final(b):
        to = lax.rem(q + off(b), n_pos)
        return remote(cd.at[0, rows(b)], fin.at[rows(q)], sf.at[b], rf.at[b], {'ep': to})

    back = [b for r in range(nh - 1, -1, -1) for b in (r, nh + r)]
    for b in back:
        n = nh + b if b < nh else b - nh
        encode(1, n, acc[1, rows(n)])
        plain(b).start()
    for r in range(nh):
        for w in range(2):
            relay(r, w).wait_recv()
    unit(2)
    for b in back:
        encode(2, b, acc[1, rows(b)])
        far(b).start()
    for r in range(nh):
        for w in range(2):
            late(r, w).wait_recv()
    unit(3)
    for b in back:
        far(b).wait_recv()
        encode(3, b, acc[1, rows(b)] + decode(rel.at[rows(b)]))
        merged(b).start()
    for b in back:
        plain(b).wait_recv()
        merged(b).wait_recv()
        encode(0, b, acc[0, rows(b)] + decode(rec.at[0, rows(b)]) + decode(rec.at[1, rows(b)]))
        if b:
            final(b).start()
        else:
            fin[rows(q)] = cd[0, rows(0)]
    for b in range(1, n_pos):
        final(b).wait_recv()
    place = pick[...].T
    scale = fin[:, d:d + 128]
    for n in range(4):
        cols = pl.ds(n * wide, wide)
        v = _decode(fin[:, cols], scale)
        total = jnp.zeros((place.shape[0], wide), jnp.float32)
        for _ in range(3):
            t = v.astype(jnp.bfloat16)
            total += jnp.dot(place, t, preferred_element_type=jnp.float32)
            v = v - t.astype(jnp.float32)
        out[:, cols] = total.astype(jnp.bfloat16)

    for b in range(n_pos):
        near(b).wait_send()
        plain(b).wait_send()
        far(b).wait_send()
        merged(b).wait_send()
        if b:
            x_send(b).wait_send()
            final(b).wait_send()
    for r in range(nh):
        for w in range(2):
            late(r, w).wait_send()
            relay(r, w).wait_send()


def _moe(x, pick, gs, w1, w3, w2, n_pos, n_tp, cap):
    n_exp, ff, d = w1.shape
    ch = n_pos * cap
    wide = d + GATE_LANES
    coded = d + 128
    dma = pltpu.SemaphoreType.DMA
    vmem = pl.BlockSpec(memory_space=pltpu.VMEM)
    hbm = pl.BlockSpec(memory_space=pl.ANY)
    return pl.pallas_call(
        functools.partial(_kernel, n_pos, n_tp, cap),
        out_shape=jax.ShapeDtypeStruct(x.shape, jnp.bfloat16),
        in_specs=[vmem, vmem, vmem, hbm, hbm, hbm],
        out_specs=vmem,
        scratch_shapes=[
            pltpu.VMEM((n_pos, cap, wide), jnp.bfloat16),
            pltpu.VMEM((4, ch, wide), jnp.bfloat16),
            pltpu.VMEM((d, ch), jnp.bfloat16),
            pltpu.VMEM((2, 2, ch, ff), jnp.bfloat16),
            pltpu.VMEM((2, ch, d), jnp.float32),
            pltpu.VMEM((4, ch, coded), jnp.int16),
            pltpu.VMEM((2, ch, coded), jnp.int16),
            pltpu.VMEM((ch, coded), jnp.int16),
            pltpu.VMEM((ch, coded), jnp.int16),
            pltpu.VMEM((n_exp // 2, 4 * ff, d), jnp.bfloat16),
            pltpu.VMEM((n_exp, ff, d), jnp.bfloat16),
            dma((n_exp, 3)),
        ] + [dma((n_pos,)) for _ in range(16)],
        compiler_params=pltpu.CompilerParams(
            collective_id=0, has_side_effects=True, vmem_limit_bytes=67043328),
    )(x, pick, gs, w1, w3, w2)


def solution(mesh):
    n_pos, n_tp = mesh.shape['ep'], mesh.shape['tp']
    rows_spec = P(('dp', 'ep', 'tp'), None)

    def body(x, idx, gate, w1, w3, w2):
        rows = x.shape[0]
        n_exp = w1.shape[0]
        cap = 2 * rows // n_pos
        pick, gs = _route(idx, gate, n_pos, n_exp, cap)
        return _moe(x, pick, gs, jnp.swapaxes(w1, 1, 2), jnp.swapaxes(w3, 1, 2), w2, n_pos, n_tp, cap)

    return jax.shard_map(body, mesh=mesh,
                         in_specs=(rows_spec, rows_spec, rows_spec,
                                   P('ep', None, 'tp'), P('ep', None, 'tp'), P('ep', 'tp', None)),
                         out_specs=rows_spec, check_vma=False)
```

```python
import functools

import jax
import jax.numpy as jnp
from jax import lax
from jax.experimental import pallas as pl
from jax.experimental.pallas import tpu as pltpu
from jax.sharding import PartitionSpec as P

MESH = pl.DeviceIdType.MESH
GATE_LANES = 128
CODE_MAX = 32700.0
TINY = 1e-37


def _encode(v):
    r, d = v.shape
    top = jnp.max(jnp.abs(v), axis=1, keepdims=True)
    e = jnp.ceil(jnp.log2(jnp.maximum(top, TINY)))
    root = v * lax.rsqrt(jnp.maximum(jnp.abs(v), TINY))
    code = jnp.round(root * (CODE_MAX * jnp.exp2(-0.5 * e))).astype(jnp.int32).astype(jnp.int16)
    return code, jnp.broadcast_to(e, (r, 128)).astype(jnp.int32).astype(jnp.int16)


def _decode(code, e):
    e = e.astype(jnp.int32).astype(jnp.float32)[:, 0:1]
    root = code.astype(jnp.int32).astype(jnp.float32) * (jnp.exp2(0.5 * e) * (1.0 / CODE_MAX))
    return root * jnp.abs(root)


def _route(ids, gates, pick, xs, n_pos, n_exp, cap, d):
    top, rows = ids.shape
    hit = jnp.concatenate(
        [jnp.max(jnp.where((ids[...] >= p * n_exp) & (ids[...] < (p + 1) * n_exp), 1.0, 0.0), axis=0, keepdims=True)
         for p in range(n_pos)], axis=0)
    below = lax.broadcasted_iota(jnp.int32, (rows, rows), 0)
    right = lax.broadcasted_iota(jnp.int32, (rows, rows), 1)
    before = jnp.where(below < right, 1.0, 0.0).astype(jnp.bfloat16)
    rank = jnp.dot(hit.astype(jnp.bfloat16), before, preferred_element_type=jnp.float32)
    slot = jnp.where(hit > 0.0, rank, -1.0).astype(jnp.int32)
    at = lax.broadcasted_iota(jnp.int32, (cap, rows), 0)
    expert = lax.broadcasted_iota(jnp.int32, (n_pos * n_exp, rows), 0)
    g = jnp.zeros((n_pos * n_exp, rows), jnp.float32)
    for k in range(top):
        g += jnp.where(ids[k:k + 1, :] == expert, gates[k:k + 1, :], 0.0)
    terms = []
    for _ in range(3):
        t = g.astype(jnp.bfloat16)
        terms.append(t)
        g = g - t.astype(jnp.float32)
    fill = jnp.zeros((GATE_LANES - 3 * n_exp, rows), jnp.bfloat16)
    for p in range(n_pos):
        one = jnp.where(at == slot[p:p + 1, :], 1.0, 0.0).astype(jnp.bfloat16)
        pick[p * cap:(p + 1) * cap, :] = one
        mine = jnp.concatenate([t[p * n_exp:(p + 1) * n_exp, :] for t in terms] + [fill], axis=0)
        gs = lax.dot_general(one, mine, (((1,), (1,)), ((), ())), preferred_element_type=jnp.float32)
        xs[p, :, d:d + GATE_LANES] = gs.astype(jnp.bfloat16)


def _kernel(n_pos, n_tp, cap, x, ids, gates, w1, w3, w2, out, pick, xs, xb, xt, hs, acc0, acc1, cd0, cd1, cd2, cd3,
            rec, rel, fin, b13, b2,
            wsem, sx, rx, sn, rn, sl, rl, sr, rr, su, ru, sg, rg, sm, rm, sf, rf):
    q = lax.axis_index('ep')
    y = lax.axis_index('tp')
    up = lax.rem(y + 1, n_tp)
    down = lax.rem(y + n_tp - 1, n_tp)
    n_exp, ff, d = w1.shape
    ch = n_pos * cap
    nh = n_pos // 2
    pairs = n_exp // 2

    def remote(src, dst, ssem, rsem, dev):
        return pltpu.make_async_remote_copy(src_ref=src, dst_ref=dst, send_sem=ssem, recv_sem=rsem,
                                            device_id=dev, device_id_type=MESH)

    def weights(e):
        i, r = e // 2, (e % 2) * 2 * ff
        return (pltpu.make_async_copy(w1.at[e], b13.at[i, pl.ds(r, ff)], wsem.at[e, 0]),
                pltpu.make_async_copy(w3.at[e], b13.at[i, pl.ds(r + ff, ff)], wsem.at[e, 1]),
                pltpu.make_async_copy(w2.at[e], b2.at[e], wsem.at[e, 2]))

    barrier = pltpu.get_barrier_semaphore()
    for k in range(1, n_pos):
        pl.semaphore_signal(barrier, inc=1, device_id={'ep': lax.rem(q + k, n_pos)}, device_id_type=MESH)
    for t in (up, down):
        pl.semaphore_signal(barrier, inc=1, device_id={'tp': t}, device_id_type=MESH)

    def load(e, carry):
        for c in weights(e):
            c.start()
        return carry

    lax.fori_loop(0, n_exp, load, 0)
    wide = d // 4
    _route(ids, gates, pick, xs, n_pos, n_exp, cap, d)
    for n in range(4):
        cols = pl.ds(n * wide, wide)
        picked = jnp.dot(pick[...], x[:, cols], preferred_element_type=jnp.float32)
        xs[:, :, cols] = picked.astype(jnp.bfloat16).reshape(n_pos, cap, wide)
    pl.semaphore_wait(barrier, n_pos + 1)

    def off(b):
        return b if b < nh else n_pos + nh - 1 - b

    def rows(n):
        return pl.ds(n * cap, cap)

    early, rest = range(nh // 2), range(nh // 2, nh)
    first4 = [b for r in early for b in (r, nh + r)]
    last4 = [b for r in rest for b in (r, nh + r)]
    units = (
        [('O', b) for b in first4] + [(c, r) for r in early for c in 'AB'],
        [(c, r) for r in rest for c in 'AB'] + [('F', b) for b in first4],
        [('F', b) for b in last4] + [(c, r) for r in early for c in 'CD'],
        [('O', b) for b in last4] + [(c, r) for r in rest for c in 'CD'],
    )
    place = {name: (u, n) for u, names in enumerate(units) for n, name in enumerate(names)}

    def spot(c, r):
        u, n = place[c, r]
        return xb.at[u, rows(n)]

    def x_send(b):
        to = lax.rem(q + n_pos - off(b), n_pos)
        return remote(xs.at[to], spot('O', b), sx.at[b], rx.at[b], {'ep': to})

    def near(b):
        src = xs.at[q] if b == 0 else spot('O', b)
        if b < nh:
            return remote(src, spot('A', b), sn.at[b], rn.at[b], {'tp': up})
        return remote(src, spot('B', b - nh), sn.at[b], rn.at[b], {'tp': down})

    def late(b):
        if b < nh:
            return remote(spot('O', b), spot('C', b), sl.at[b], rl.at[b], {'tp': down})
        return remote(spot('O', b), spot('D', b - nh), sl.at[b], rl.at[b], {'tp': up})

    def relay(b):
        if b < nh:
            return remote(spot('A', b), spot('F', b), sr.at[b], rr.at[b], {'tp': up})
        return remote(spot('B', b - nh), spot('F', b), sr.at[b], rr.at[b], {'tp': down})

    for b in (first4 + last4)[1:]:
        x_send(b).start()
    near(0).start()
    u, n = place['O', 0]
    xb[u, rows(n)] = xs[q]
    for b in first4[1:]:
        x_send(b).wait_recv()
        near(b).start()
    for b in first4:
        near(b).wait_recv()

    lane = lax.broadcasted_iota(jnp.int32, (ch, GATE_LANES), 1)

    def unit(u, acc, hook=None):
        for n in range(4):
            cols = pl.ds(n * wide, wide)
            xt[cols, :] = xb[u, :, cols].T

        def gate(gv, e):
            mine = (lane == e) | (lane == e + n_exp) | (lane == e + 2 * n_exp)
            return jnp.sum(jnp.where(mine, gv, 0.0), axis=1, keepdims=True)

        def up_proj(i):
            if hook is not None:
                hook(i)
            return jnp.dot(b13[i], xt[...], preferred_element_type=jnp.float32)

        def hidden(i, ab):
            for t in range(2):
                a, b = ab[2 * t * ff:(2 * t + 1) * ff], ab[(2 * t + 1) * ff:(2 * t + 2) * ff]
                hs[lax.rem(i, 2), t] = (a * jax.nn.sigmoid(a) * b).astype(jnp.bfloat16).T

        def down_proj(i):
            gv = xb[u, :, d:d + GATE_LANES].astype(jnp.float32)
            g0, g1 = gate(gv, 2 * i), gate(gv, 2 * i + 1)
            p = lax.rem(i, 2)
            for n in range(4):
                cols = pl.ds(n * wide, wide)
                o0 = jnp.dot(hs[p, 0], b2[2 * i, :, cols], preferred_element_type=jnp.float32)
                o1 = jnp.dot(hs[p, 1], b2[2 * i + 1, :, cols], preferred_element_type=jnp.float32)
                acc[:, cols] = jnp.where(i == 0, 0.0, acc[:, cols]) + (g0 * o0 + g1 * o1)

        def pair(i, carry):
            ab = up_proj(i + 1)
            down_proj(i)
            hidden(i + 1, ab)
            return carry

        hidden(0, up_proj(0))
        lax.fori_loop(0, pairs - 1, pair, 0)
        down_proj(pairs - 1)

    def relays(r):
        relay(r).start()
        relay(nh + r).start()

    def nears(r):
        for b in (r, nh + r):
            x_send(b).wait_recv()
            near(b).start()

    def lates(r):
        late(r).start()
        late(nh + r).start()

    def passed(r):
        near(r).wait_recv()
        near(nh + r).wait_recv()
        relays(r)

    todo = [functools.partial(f, r) for f, r in (
        (relays, 0), (nears, 2), (relays, 1), (nears, 3), (lates, 0), (lates, 1), (passed, 2), (passed, 3))]

    def first(i):
        for t in range(2):
            for c in weights(2 * i + t):
                c.wait()
        for step, act in enumerate(todo):
            pl.when(i == step)(act)

    def encode(ref, n, v):
        ref[rows(n), 0:d], ref[rows(n), d:d + 128] = _encode(v)

    def decode(ref):
        return _decode(ref[:, 0:d], ref[:, d:d + 128])

    def mine(c, r):
        u, n = place[c, r]
        return (acc1 if u else acc0)[rows(n), :]

    def plain(b):
        w = 1 if b < nh else 0
        return remote(cd1.at[rows(b)], rec.at[w, rows(b)], su.at[b], ru.at[b], {'tp': down if w else up})

    def far(b):
        return remote(cd2.at[rows(b)], rel.at[rows(b)], sg.at[b], rg.at[b], {'tp': up if b < nh else down})

    def merged(b):
        w = 0 if b < nh else 1
        return remote(cd3.at[rows(b)], rec.at[w, rows(b)], sm.at[b], rm.at[b], {'tp': down if w else up})

    def final(b):
        to = lax.rem(q + off(b), n_pos)
        return remote(cd0.at[rows(b)], fin.at[rows(q)], sf.at[b], rf.at[b], {'ep': to})

    def send_plain(blocks):
        for b in blocks:
            encode(cd1, b, mine('A', b) if b < nh else mine('B', b - nh))
            plain(b).start()

    def send_far(blocks):
        for b in blocks:
            encode(cd2, b, mine('F', b))
            far(b).start()

    def send_merged(blocks):
        for b in blocks:
            far(b).wait_recv()
            own = mine('C', b) if b < nh else mine('D', b - nh)
            encode(cd3, b, own + decode(rel.at[rows(b)]))
            merged(b).start()

    def send_final(blocks):
        for b in blocks:
            plain(b).wait_recv()
            merged(b).wait_recv()
            encode(cd0, b, mine('O', b) + decode(rec.at[0, rows(b)]) + decode(rec.at[1, rows(b)]))
            if b:
                final(b).start()
            else:
                fin[rows(q)] = cd0[rows(0)]

    unit(0, acc0, first)
    send_plain(first4)
    lates(2)
    lates(3)
    for b in first4:
        relay(b).wait_recv()
    unit(1, acc1)
    send_far(first4)
    send_plain(last4)
    for b in last4:
        relay(b).wait_recv()
    for b in first4:
        late(b).wait_recv()
    unit(2, acc1)
    send_far(last4)
    send_merged(first4)
    for b in last4:
        late(b).wait_recv()
    unit(3, acc1)
    send_merged(last4)
    send_final(first4)
    send_final(last4)
    for b in range(1, n_pos):
        final(b).wait_recv()
    home = pick[...].T
    scale = fin[:, d:d + 128]
    for n in range(4):
        cols = pl.ds(n * wide, wide)
        v = _decode(fin[:, cols], scale)
        total = jnp.zeros((home.shape[0], wide), jnp.float32)
        for _ in range(3):
            t = v.astype(jnp.bfloat16)
            total += jnp.dot(home, t, preferred_element_type=jnp.float32)
            v = v - t.astype(jnp.float32)
        out[:, cols] = total.astype(jnp.bfloat16)

    for b in range(n_pos):
        near(b).wait_send()
        late(b).wait_send()
        relay(b).wait_send()
        plain(b).wait_send()
        far(b).wait_send()
        merged(b).wait_send()
        if b:
            x_send(b).wait_send()
            final(b).wait_send()


def _moe(x, ids, gates, w1, w3, w2, n_pos, n_tp, cap):
    n_exp, ff, d = w1.shape
    ch = n_pos * cap
    wide = d + GATE_LANES
    coded = d + 128
    dma = pltpu.SemaphoreType.DMA
    vmem = pl.BlockSpec(memory_space=pltpu.VMEM)
    hbm = pl.BlockSpec(memory_space=pl.ANY)
    return pl.pallas_call(
        functools.partial(_kernel, n_pos, n_tp, cap),
        out_shape=jax.ShapeDtypeStruct(x.shape, jnp.bfloat16),
        in_specs=[vmem, vmem, vmem, hbm, hbm, hbm],
        out_specs=vmem,
        scratch_shapes=[
            pltpu.VMEM((ch, x.shape[0]), jnp.bfloat16),
            pltpu.VMEM((n_pos, cap, wide), jnp.bfloat16),
            pltpu.VMEM((4, ch, wide), jnp.bfloat16),
            pltpu.VMEM((d, ch), jnp.bfloat16),
            pltpu.VMEM((2, 2, ch, ff), jnp.bfloat16),
            pltpu.VMEM((ch, d), jnp.float32),
            pltpu.VMEM((ch, d), jnp.float32),
            pltpu.VMEM((ch, coded), jnp.int16),
            pltpu.VMEM((ch, coded), jnp.int16),
            pltpu.VMEM((ch, coded), jnp.int16),
            pltpu.VMEM((ch, coded), jnp.int16),
            pltpu.VMEM((2, ch, coded), jnp.int16),
            pltpu.VMEM((ch, coded), jnp.int16),
            pltpu.VMEM((ch, coded), jnp.int16),
            pltpu.VMEM((n_exp // 2, 4 * ff, d), jnp.bfloat16),
            pltpu.VMEM((n_exp, ff, d), jnp.bfloat16),
            dma((n_exp, 3)),
        ] + [dma((n_pos,)) for _ in range(16)],
        compiler_params=pltpu.CompilerParams(
            collective_id=0, has_side_effects=True, vmem_limit_bytes=67043328),
    )(x, ids, gates, w1, w3, w2)


def solution(mesh):
    n_pos, n_tp = mesh.shape['ep'], mesh.shape['tp']
    rows_spec = P(('dp', 'ep', 'tp'), None)

    def body(x, idx, gate, w1, w3, w2):
        rows = x.shape[0]
        cap = 2 * rows // n_pos
        return _moe(x, idx.T, gate.T, jnp.swapaxes(w1, 1, 2), jnp.swapaxes(w3, 1, 2), w2, n_pos, n_tp, cap)

    return jax.shard_map(body, mesh=mesh,
                         in_specs=(rows_spec, rows_spec, rows_spec,
                                   P('ep', None, 'tp'), P('ep', None, 'tp'), P('ep', 'tp', None)),
                         out_specs=rows_spec, check_vma=False)
```
